32 devices in a mesh: groups: 2 (over x), seq: 16 (over z, y, core).
Axes of the slice: x: 2, y: 2, z: 4, core: 2. Of those that a mesh axis runs over, the one named last changes fastest.
Arguments:
- queries: bfloat16 [64, 128, 576], P('groups', 'seq'), parts along dimension 0, may hold values from -8 to 8
- prefix_pool: bfloat16 [1024, 64, 576], P(('groups', 'seq')), parts along dimension 0, may hold values from -6 to 6
- block_table: int32 [8, 128], P('groups'), parts along dimension 0, may hold values from 0 to 511, as said below
- prefix_of: int32 [64], P('groups'), parts along dimension 0, may hold values from 0 to 3
- suffix_cache: bfloat16 [64, 2048, 576], P('groups', 'seq'), parts along dimension 0, may hold values from -24 to 24
- suffix_len: int32 [64], P('groups'), parts along dimension 0, may hold values from 2 to 2048
Outputs:
- context: bfloat16 [64, 128, 512], P('groups', 'seq'), parts along dimension 0
The draws below stay inside these ranges and needn't reach their ends.
There are 2 independent parts, one for each index of `groups`. The reference program is written for one: setup_inputs(seed, part) draws one part's arguments, and reference() takes and returns one part's arrays. A program takes and returns all parts, laid end to end along the dimension named above; each array names one. Nothing has to cross between parts.
Inputs may be any that keep to these rules, and one draw needn't show every extreme that they name: `block_table`: each of the 512 pool blocks is named exactly once in the table, and of each aligned run of 32 pool blocks exactly 8 belong to each prefix.
All inputs are finite; a program needn't handle non-finite values.
Results may differ from the reference program's by a relative error of at most 0.0033.
Values may be sent and summed in bfloat16 or wider, within the bound.
A program may use at most 128 MiB of HBM per device.

```python
import jax
import jax.numpy as jnp
from jax import lax

LAT = 512
ROPE = 64
HEADS = 128
BLK = 64
PREFIXES = 4
BLK_DEV = 32
REQS = 32
NBLK = 512
PBLK = 128
PLEN = 8192
SUF_MAX = 2048


def base_queries(key):
    values = 1.75 * jax.random.normal(jax.random.fold_in(key, 11), (REQS, HEADS, LAT + ROPE), jnp.float32)
    return jnp.clip(values, -8.0, 8.0)


def draw_queries(key, part):
    return base_queries(key).astype(jnp.bfloat16)


def draw_prefix_of(key, part):
    chosen = jax.random.randint(jax.random.fold_in(key, 21), (REQS,), 0, PREFIXES, dtype=jnp.int32)
    step_size = jax.random.randint(jax.random.fold_in(key, 22), (), 1, PREFIXES, dtype=jnp.int32)
    first = (chosen[1] + step_size) % PREFIXES
    return chosen.at[0].set(first).astype(jnp.int32)


def draw_suffix_cache(key, part):
    suffix_rows = jax.random.normal(jax.random.fold_in(key, 12), (REQS, SUF_MAX, LAT + ROPE), jnp.float32)
    return jnp.clip(suffix_rows, -24.0, 24.0).astype(jnp.bfloat16)


def draw_block_table(key, part):
    holders = NBLK // BLK_DEV
    base = jnp.arange(BLK_DEV, dtype=jnp.int32) % PREFIXES
    device_keys = jax.random.split(jax.random.fold_in(key, 13), holders)
    labels = jax.vmap(lambda one: jax.random.permutation(one, base))(device_keys).reshape(NBLK)
    ranks = jax.random.permutation(jax.random.fold_in(key, 15), NBLK).astype(jnp.int32)
    ordered = jnp.argsort(labels * NBLK + ranks)
    return ordered.reshape(PREFIXES, PBLK).astype(jnp.int32)


def set_ends(values, own_key, low, top_value):
    shape = values.shape
    place = [jax.random.randint(jax.random.fold_in(own_key, axis), (), 0, shape[axis]) for axis in range(len(shape))]
    values = values.at[tuple(place)].set(low)
    longest = shape.index(max(shape))
    place[longest] = (place[longest] + 1) % shape[longest]
    return values.at[tuple(place)].set(top_value)


def block_levels(stream_key, shape, shards, least, high):
    gain = 1.0
    for position, shards_of in shards:
        heights = jax.random.uniform(jax.random.fold_in(jax.random.fold_in(stream_key, 6), position), (shards_of,), jnp.float32, least / len(shards), high / len(shards))
        gain = gain * jnp.repeat(jnp.exp(heights), shape[position] // shards_of).reshape((-1,) + (1,) * (len(shape) - 1 - position))
    return gain


def centred(own_key, dims, deviation, bound, pieces=(), kind=jnp.bfloat16):
    gain = block_levels(own_key, dims, pieces, -0.22, 0.18) if pieces else 1.0
    values = jax.random.normal(own_key, dims, jnp.float32) * deviation * gain
    return jnp.minimum(jnp.maximum(values, -bound), bound).astype(kind)


def setup_inputs(seed: int = 0, part: int = 0) -> dict:
    arg_keys = jax.random.split(jax.random.key(seed), 7)
    part_keys = jax.random.split(jax.random.fold_in(arg_keys[6], part), 7)
    return {
        "queries": draw_queries(jax.random.fold_in(jax.random.fold_in(arg_keys[6], part), 71), part),
        "prefix_pool": centred(part_keys[1], (NBLK, BLK, LAT + ROPE), 1.0, 6.0, ((0, 16),)),
        "block_table": draw_block_table(jax.random.fold_in(jax.random.fold_in(arg_keys[6], part), 71), part),
        "prefix_of": draw_prefix_of(jax.random.fold_in(jax.random.fold_in(arg_keys[6], part), 71), part),
        "suffix_cache": draw_suffix_cache(jax.random.fold_in(jax.random.fold_in(arg_keys[6], part), 71), part),
        "suffix_len": set_ends(jax.random.randint(part_keys[5], (REQS,), 2, SUF_MAX + 1), jax.random.fold_in(part_keys[5], 1), 2, SUF_MAX).astype(jnp.int32),
    }


score_scale = 192.0 ** -0.5


def single(packed, prefix_pool, block_table):
    query_rows, chosen, suffix_rows, length = packed
    blocks = block_table[chosen]
    prefix_keys = prefix_pool[blocks].reshape(PLEN, LAT + ROPE)
    prefix_scores = jnp.dot(query_rows, prefix_keys.T, preferred_element_type=jnp.float32) * score_scale
    suffix_scores = jnp.dot(query_rows, suffix_rows.T, preferred_element_type=jnp.float32) * score_scale
    live_slots = jnp.arange(SUF_MAX, dtype=jnp.int32) < length
    suffix_scores = jnp.where(live_slots[None, :], suffix_scores, -jnp.inf)
    highest = jnp.maximum(jnp.max(prefix_scores, axis=1), jnp.max(suffix_scores, axis=1))
    prefix_weights = jnp.exp(prefix_scores - highest[:, None])
    suffix_weights = jnp.exp(suffix_scores - highest[:, None])
    weight_sum = jnp.sum(prefix_weights, axis=1) + jnp.sum(suffix_weights, axis=1)
    weighted = jnp.dot(prefix_weights.astype(jnp.bfloat16), prefix_keys[:, :LAT], preferred_element_type=jnp.float32)
    weighted = weighted + jnp.dot(suffix_weights.astype(jnp.bfloat16), suffix_rows[:, :LAT], preferred_element_type=jnp.float32)
    return (weighted / weight_sum[:, None]).astype(jnp.bfloat16)


def reference(queries, prefix_pool, block_table, prefix_of, suffix_cache, suffix_len):
    return lax.map(lambda packed: single(packed, prefix_pool, block_table), (queries, prefix_of, suffix_cache, suffix_len))
```

```python
import functools

import jax
import jax.numpy as jnp
from jax import lax
from jax.experimental import pallas as pl
from jax.experimental.pallas import tpu as pltpu
from jax.sharding import PartitionSpec as P

LAT = 512


score_scale = 192.0 ** (-0.5)


def body(queries, prefix_pool, block_table, prefix_of, suffix_cache, suffix_len):
    blocks_here, block_rows, channels = prefix_pool.shape
    prefix_total = block_table.shape[0]
    slots_here = suffix_cache.shape[1]
    position = lax.axis_index("seq")
    block_ids = position * blocks_here + lax.iota(jnp.int32, blocks_here)
    owners = jnp.any(block_table[:, :, None] == block_ids[None, None, :], axis=1)
    prefix_ids = lax.iota(jnp.int32, prefix_total)
    labels = jnp.sum(owners.astype(jnp.int32) * prefix_ids[:, None], axis=0)
    order = jnp.argsort(labels, stable=True)
    segment_rows = blocks_here // prefix_total * block_rows
    segments = prefix_pool[order].reshape(prefix_total, segment_rows, channels)
    request_keys = jnp.concatenate([segments[prefix_of], suffix_cache], axis=1)
    slot_ids = position * slots_here + lax.iota(jnp.int32, slots_here)
    live_slots = slot_ids[None, :] < suffix_len[:, None]
    visible = jnp.concatenate(
        [jnp.ones((live_slots.shape[0], segment_rows), bool), live_slots], axis=1
    )
    scores = (
        jnp.einsum(
            "rhw,rkw->rhk",
            lax.all_gather(queries, "seq", axis=1, tiled=True),
            request_keys,
            preferred_element_type=jnp.float32,
        )
        * score_scale
    )
    scores = jnp.where(visible[:, None, :], scores, -jnp.inf)
    highest = lax.pmax(jnp.max(scores, axis=2), "seq")
    weights = jnp.exp(scores - highest[:, :, None])
    weight_sum = jnp.sum(weights, axis=2)
    rounded = weights.astype(jnp.bfloat16)
    weighted = jnp.einsum(
        "rhk,rkl->rhl", rounded, request_keys[:, :, :LAT], preferred_element_type=jnp.float32
    )
    weight_sum, weighted = (
        lax.psum_scatter(weight_sum, "seq", scatter_dimension=1, tiled=True),
        lax.psum_scatter(weighted, "seq", scatter_dimension=1, tiled=True),
    )
    return (weighted / weight_sum[:, :, None]).astype(jnp.bfloat16)


MESH = pl.DeviceIdType.MESH
REQ_CHUNK = 4


def kernel(
    chips,
    order_ref,
    prefix_ref,
    length_ref,
    q_hbm,
    pool_hbm,
    suffix_hbm,
    out_ref,
    pool_v,
    suffix_v,
    q_v,
    o_s,
    stat_s,
    o_r,
    stat_r,
    local_sem,
    pool_sem,
    suf_sem,
    q_send,
    q_recv,
    o_send,
    o_recv,
    t_send,
    t_recv,
):
    group = lax.axis_index("groups")
    position = lax.axis_index("seq")
    core = lax.rem(position, 2)
    me = lax.div(position, 2)
    column = lax.rem(me, 2)
    depth = chips // 2
    row = lax.div(me, 2)
    partner = position + 1 - 2 * core
    across = me + 1 - 2 * column

    def device(chip):
        return (group, chip * 2 + core)

    def chip_at(step):
        return lax.rem(me + step, chips)

    def row_at(step):
        return lax.rem(row + step, depth) * 2 + column

    blocks = pool_hbm.shape[0]
    requests = suffix_hbm.shape[0]
    slots = suffix_hbm.shape[1]
    pairs = q_hbm.shape[0]
    heads = q_hbm.shape[1] // 2
    chunks = requests // REQ_CHUNK
    chunk_pairs = REQ_CHUNK // 2

    barrier = pltpu.get_barrier_semaphore()
    pl.semaphore_signal(barrier, inc=1, device_id=(group, partner), device_id_type=MESH)
    for step in range(1, chips):
        pl.semaphore_signal(
            barrier, inc=1, device_id=device(chip_at(step)), device_id_type=MESH
        )

    def rows_of(c):
        return pl.ds(c * chunk_pairs, chunk_pairs)

    def reqs_of(c):
        return pl.ds(c * REQ_CHUNK, REQ_CHUNK)

    def q_local():
        return pltpu.make_async_copy(q_hbm, q_v.at[me], local_sem.at[0])

    def pool_local():
        return pltpu.make_async_copy(pool_hbm, pool_v.at[core], local_sem.at[1])

    def suffix_local(c):
        return pltpu.make_async_copy(
            suffix_hbm.at[reqs_of(c)], suffix_v.at[core, reqs_of(c)], local_sem.at[2 + c]
        )

    def q_copy(c, step):
        dest = across if step == 0 else row_at(step)
        return pltpu.make_async_remote_copy(
            src_ref=q_hbm.at[rows_of(c)],
            dst_ref=q_v.at[me, rows_of(c)],
            send_sem=q_send.at[step, c],
            recv_sem=q_recv.at[step, c],
            device_id=device(dest),
            device_id_type=MESH,
        )

    def q_forward(c, step):
        source = row_at(depth - step)
        return pltpu.make_async_remote_copy(
            src_ref=q_v.at[source, rows_of(c)],
            dst_ref=q_v.at[source, rows_of(c)],
            send_sem=q_send.at[depth - 1 + step, c],
            recv_sem=q_recv.at[depth - 1 + step, c],
            device_id=device(across),
            device_id_type=MESH,
        )

    def pool_remote():
        return pltpu.make_async_remote_copy(
            src_ref=pool_hbm,
            dst_ref=pool_v.at[core],
            send_sem=pool_sem.at[0],
            recv_sem=pool_sem.at[1],
            device_id=(group, partner),
            device_id_type=MESH,
        )

    def suffix_remote(c):
        return pltpu.make_async_remote_copy(
            src_ref=suffix_hbm.at[reqs_of(c)],
            dst_ref=suffix_v.at[core, reqs_of(c)],
            send_sem=suf_sem.at[0, c],
            recv_sem=suf_sem.at[1, c],
            device_id=(group, partner),
            device_id_type=MESH,
        )

    def o_copy(c, step):
        dest = chip_at(step)
        return pltpu.make_async_remote_copy(
            src_ref=o_s.at[dest, rows_of(c)],
            dst_ref=o_r.at[me, rows_of(c)],
            send_sem=o_send.at[step, c],
            recv_sem=o_recv.at[step, c],
            device_id=device(dest),
            device_id_type=MESH,
        )

    def t_copy(c, step):
        dest = chip_at(step)
        return pltpu.make_async_remote_copy(
            src_ref=stat_s.at[dest, c],
            dst_ref=stat_r.at[me, c],
            send_sem=t_send.at[step, c],
            recv_sem=t_recv.at[step, c],
            device_id=device(dest),
            device_id_type=MESH,
        )

    def o_local(c):
        return pltpu.make_async_copy(
            o_s.at[me, rows_of(c)], o_r.at[me, rows_of(c)], o_send.at[0, c]
        )

    def t_local(c):
        return pltpu.make_async_copy(stat_s.at[me, c], stat_r.at[me, c], t_send.at[0, c])

    def loop(count, body):
        def step(c, carry):
            body(c)
            return carry

        lax.fori_loop(0, count, step, 0)

    q_local().start()
    pool_local().start()
    loop(chunks, lambda c: suffix_local(c).start())
    pl.semaphore_wait(barrier, chips)

    pool_remote().start()

    def start_q(c):
        for step in range(1, depth):
            q_copy(c, step).start()
        q_copy(c, 0).start()
        suffix_remote(c).start()

    loop(chunks, start_q)

    def forward(c):
        for step in range(1, depth):
            q_copy(c, step).wait_recv()
            q_forward(c, step).start()

    forward(0)
    q_local().wait()
    pool_local().wait()
    pool_remote().wait()

    lanes = lax.broadcasted_iota(jnp.int32, (chips * heads, 128), 1)
    slot_ids = lax.broadcasted_iota(jnp.int32, (1, 2 * slots), 1) + me * (2 * slots)
    prefixes = order_ref.shape[1]
    per_prefix = blocks // prefixes

    def attend(q, request):
        chosen = prefix_ref[request]
        parts = []
        for side in range(2):
            for k in range(per_prefix):
                parts.append(pool_v[side, order_ref[side * per_prefix + k, chosen]])
        parts.append(suffix_v[0, request])
        parts.append(suffix_v[1, request])
        keys = jnp.concatenate(parts, axis=0)
        scores = (
            lax.dot_general(
                q, keys, (((1,), (1,)), ((), ())), preferred_element_type=jnp.float32
            )
            * score_scale
        )
        split = keys.shape[0] - 2 * slots
        live = slot_ids < length_ref[request]
        scores = jnp.concatenate(
            [scores[:, :split], jnp.where(live, scores[:, split:], -jnp.inf)], axis=1
        )
        highest = jnp.max(scores, axis=1, keepdims=True)
        weights = jnp.exp(scores - highest)
        total = jnp.sum(weights, axis=1, keepdims=True)
        mixed = jnp.dot(
            weights.astype(jnp.bfloat16), keys[:, :LAT], preferred_element_type=jnp.float32
        )
        return mixed / total, highest, total

    def do_chunk(c):
        @pl.when(c + 1 < chunks)
        def _():
            forward(c + 1)

        q_copy(c, 0).wait_recv()
        for step in range(1, depth):
            q_forward(c, step).wait_recv()
        suffix_local(c).wait()
        suffix_remote(c).wait()
        stats = jnp.zeros((chips * heads, 128), jnp.float32)
        for half in range(chunk_pairs):
            pair = c * chunk_pairs + half
            q = q_v[:, pair].astype(jnp.float32).reshape(chips, 2, heads, q_v.shape[-1])
            outs = []
            for i in range(2):
                request = pair * 2 + i
                one = q[:, i].reshape(chips * heads, q_v.shape[-1]).astype(jnp.bfloat16)
                mixed, highest, total = attend(one, request)
                at = 2 * (half * 2 + i)
                stats = jnp.where(lanes == at, highest, stats)
                stats = jnp.where(lanes == at + 1, total, stats)
                outs.append(mixed.reshape(chips, heads, LAT))
            both = jnp.concatenate(outs, axis=1)
            o_s[:, pair] = both.astype(jnp.bfloat16)
        stat_s[:, c] = stats.reshape(chips, heads, 128)
        for step in range(1, chips):
            o_copy(c, step).start()
            t_copy(c, step).start()
        o_local(c).start()
        t_local(c).start()

    loop(chunks, do_chunk)

    def finish(c):
        o_local(c).wait()
        t_local(c).wait()
        for step in range(1, chips):
            o_copy(c, step).wait_recv()
            t_copy(c, step).wait_recv()
        stats = stat_r[:, c]
        for half in range(chunk_pairs):
            pair = c * chunk_pairs + half
            both = o_r[:, pair].astype(jnp.float32)
            outs = []
            for i in range(2):
                at = 2 * (half * 2 + i)
                top = stats[:, :, at : at + 1]
                share = jnp.exp(top - jnp.max(top, axis=0, keepdims=True)) * stats[:, :, at + 1 : at + 2]
                share = share / jnp.sum(share, axis=0, keepdims=True)
                outs.append(jnp.sum(both[:, i * heads : (i + 1) * heads] * share, axis=0))
            out_ref[pair] = jnp.concatenate(outs, axis=0).astype(jnp.bfloat16)

    loop(chunks, finish)

    def drain(c):
        for step in range(depth):
            q_copy(c, step).wait_send()
        for step in range(1, depth):
            q_forward(c, step).wait_send()
        for step in range(1, chips):
            o_copy(c, step).wait_send()
            t_copy(c, step).wait_send()

    loop(chunks, drain)


def fused_body(seq, queries, prefix_pool, block_table, prefix_of, suffix_cache, suffix_len):
    blocks_here, block_rows, channels = prefix_pool.shape
    prefix_total = block_table.shape[0]
    requests, heads, _ = queries.shape
    slots = suffix_cache.shape[1]
    per_prefix = blocks_here // prefix_total
    chips = seq // 2
    chunks = requests // REQ_CHUNK
    pairs = requests // 2
    chip = lax.axis_index("seq") // 2

    sides = chip * 2 + lax.iota(jnp.int32, 2)
    here = (block_table // blocks_here)[None] == sides[:, None, None]
    before = jnp.tril(jnp.ones((block_table.shape[1],) * 2, jnp.int32), -1)
    rank = jnp.sum(here[:, :, None, :] * before, axis=3)
    pick = here[:, None] & (rank[:, None] == lax.iota(jnp.int32, per_prefix)[None, :, None, None])
    local = block_table - block_table // blocks_here * blocks_here
    order = jnp.sum(jnp.where(pick, local[None, None], 0), axis=3).reshape(2 * per_prefix, prefix_total)

    any_spec = pl.BlockSpec(memory_space=pltpu.HBM)
    smem = pl.BlockSpec(memory_space=pltpu.SMEM)
    dma = pltpu.SemaphoreType.DMA
    out = pl.pallas_call(
        functools.partial(kernel, chips),
        out_shape=jax.ShapeDtypeStruct((pairs, 2 * heads, LAT), jnp.bfloat16),
        in_specs=[smem, smem, smem, any_spec, any_spec, any_spec],
        out_specs=pl.BlockSpec(memory_space=pltpu.VMEM),
        scratch_shapes=[
            pltpu.VMEM((2, blocks_here, block_rows, channels), jnp.bfloat16),
            pltpu.VMEM((2, requests, slots, channels), jnp.bfloat16),
            pltpu.VMEM((chips, pairs, 2 * heads, channels), jnp.bfloat16),
            pltpu.VMEM((chips, pairs, 2 * heads, LAT), jnp.bfloat16),
            pltpu.VMEM((chips, chunks, heads, 128), jnp.float32),
            pltpu.VMEM((chips, pairs, 2 * heads, LAT), jnp.bfloat16),
            pltpu.VMEM((chips, chunks, heads, 128), jnp.float32),
            dma((2 + chunks,)),
            dma((2,)),
            dma((2, chunks)),
            dma((chips, chunks)),
            dma((chips, chunks)),
            dma((chips, chunks)),
            dma((chips, chunks)),
            dma((chips, chunks)),
            dma((chips, chunks)),
        ],
        compiler_params=pltpu.CompilerParams(
            collective_id=0, has_side_effects=True, vmem_limit_bytes=50 * 1024 * 1024
        ),
    )(
        order,
        prefix_of,
        suffix_len,
        queries.reshape(pairs, 2 * heads, channels),
        prefix_pool,
        suffix_cache,
    )
    return out.reshape(requests, heads, LAT)


def solution(mesh):
    seq = mesh.shape["seq"]
    wide = seq == 16
    local = functools.partial(fused_body, seq) if wide else body
    return jax.shard_map(
        local,
        mesh=mesh,
        in_specs=(
            P("groups", "seq", None),
            P(("groups", "seq"), None, None),
            P("groups", None),
            P("groups"),
            P("groups", "seq", None),
            P("groups"),
        ),
        out_specs=P("groups", "seq", None),
        check_vma=False,
    )
```

```python
import functools

import jax
import jax.numpy as jnp
from jax import lax
from jax.experimental import pallas as pl
from jax.experimental.pallas import tpu as pltpu
from jax.sharding import PartitionSpec as P

LAT = 512


score_scale = 192.0 ** (-0.5)


def body(queries, prefix_pool, block_table, prefix_of, suffix_cache, suffix_len):
    blocks_here, block_rows, channels = prefix_pool.shape
    prefix_total = block_table.shape[0]
    slots_here = suffix_cache.shape[1]
    position = lax.axis_index("seq")
    block_ids = position * blocks_here + lax.iota(jnp.int32, blocks_here)
    owners = jnp.any(block_table[:, :, None] == block_ids[None, None, :], axis=1)
    prefix_ids = lax.iota(jnp.int32, prefix_total)
    labels = jnp.sum(owners.astype(jnp.int32) * prefix_ids[:, None], axis=0)
    order = jnp.argsort(labels, stable=True)
    segment_rows = blocks_here // prefix_total * block_rows
    segments = prefix_pool[order].reshape(prefix_total, segment_rows, channels)
    request_keys = jnp.concatenate([segments[prefix_of], suffix_cache], axis=1)
    slot_ids = position * slots_here + lax.iota(jnp.int32, slots_here)
    live_slots = slot_ids[None, :] < suffix_len[:, None]
    visible = jnp.concatenate(
        [jnp.ones((live_slots.shape[0], segment_rows), bool), live_slots], axis=1
    )
    scores = (
        jnp.einsum(
            "rhw,rkw->rhk",
            lax.all_gather(queries, "seq", axis=1, tiled=True),
            request_keys,
            preferred_element_type=jnp.float32,
        )
        * score_scale
    )
    scores = jnp.where(visible[:, None, :], scores, -jnp.inf)
    highest = lax.pmax(jnp.max(scores, axis=2), "seq")
    weights = jnp.exp(scores - highest[:, :, None])
    weight_sum = jnp.sum(weights, axis=2)
    rounded = weights.astype(jnp.bfloat16)
    weighted = jnp.einsum(
        "rhk,rkl->rhl", rounded, request_keys[:, :, :LAT], preferred_element_type=jnp.float32
    )
    weight_sum, weighted = (
        lax.psum_scatter(weight_sum, "seq", scatter_dimension=1, tiled=True),
        lax.psum_scatter(weighted, "seq", scatter_dimension=1, tiled=True),
    )
    return (weighted / weight_sum[:, :, None]).astype(jnp.bfloat16)


MESH = pl.DeviceIdType.MESH
REQ_CHUNK = 4
LAG = 2


def kernel(
    chips,
    order_ref,
    prefix_ref,
    length_ref,
    q_hbm,
    pool_hbm,
    suffix_hbm,
    out_ref,
    pool_v,
    suffix_v,
    q_v,
    kept_v,
    kept_stat,
    y_s,
    ystat_s,
    y_r,
    ystat_r,
    z_s,
    zstat_s,
    z_r,
    zstat_r,
    local_sem,
    pool_sem,
    suf_sem,
    q_send,
    q_recv,
    y_sem,
    z_sem,
):
    group = lax.axis_index("groups")
    position = lax.axis_index("seq")
    core = lax.rem(position, 2)
    me = lax.div(position, 2)
    column = lax.rem(me, 2)
    depth = chips // 2
    row = lax.div(me, 2)
    partner = position + 1 - 2 * core
    across = me + 1 - 2 * column

    def device(chip):
        return (group, chip * 2 + core)

    def chip_at(step):
        return lax.rem(me + step, chips)

    def row_at(step):
        return lax.rem(row + step, depth) * 2 + column

    blocks = pool_hbm.shape[0]
    requests = suffix_hbm.shape[0]
    slots = suffix_hbm.shape[2]
    pairs = q_hbm.shape[0]
    heads = q_hbm.shape[1] // 2
    chunks = requests // REQ_CHUNK
    chunk_pairs = REQ_CHUNK // 2

    barrier = pltpu.get_barrier_semaphore()
    pl.semaphore_signal(barrier, inc=1, device_id=(group, partner), device_id_type=MESH)
    for step in range(1, chips):
        pl.semaphore_signal(
            barrier, inc=1, device_id=device(chip_at(step)), device_id_type=MESH
        )

    def rows_of(c):
        return pl.ds(c * chunk_pairs, chunk_pairs)

    def reqs_of(c):
        return pl.ds(c * REQ_CHUNK, REQ_CHUNK)

    def q_local():
        return pltpu.make_async_copy(q_hbm, q_v.at[0, row], local_sem.at[0])

    def pool_local():
        return pltpu.make_async_copy(pool_hbm, pool_v.at[core], local_sem.at[1])

    def suffix_local(c):
        return pltpu.make_async_copy(
            suffix_hbm.at[reqs_of(c)], suffix_v.at[core, reqs_of(c)], local_sem.at[2 + c]
        )

    def q_copy(c, step):
        dest = across if step == 0 else row_at(step)
        return pltpu.make_async_remote_copy(
            src_ref=q_hbm.at[rows_of(c)],
            dst_ref=q_v.at[1 if step == 0 else 0, row, rows_of(c)],
            send_sem=q_send.at[step, c],
            recv_sem=q_recv.at[step, c],
            device_id=device(dest),
            device_id_type=MESH,
        )

    def q_forward(c, step):
        source = lax.rem(row + depth - step, depth)
        return pltpu.make_async_remote_copy(
            src_ref=q_v.at[0, source, rows_of(c)],
            dst_ref=q_v.at[1, source, rows_of(c)],
            send_sem=q_send.at[depth - 1 + step, c],
            recv_sem=q_recv.at[depth - 1 + step, c],
            device_id=device(across),
            device_id_type=MESH,
        )

    def pool_remote():
        return pltpu.make_async_remote_copy(
            src_ref=pool_hbm,
            dst_ref=pool_v.at[core],
            send_sem=pool_sem.at[0],
            recv_sem=pool_sem.at[1],
            device_id=(group, partner),
            device_id_type=MESH,
        )

    def suffix_remote(c):
        return pltpu.make_async_remote_copy(
            src_ref=suffix_hbm.at[reqs_of(c)],
            dst_ref=suffix_v.at[core, reqs_of(c)],
            send_sem=suf_sem.at[0, c],
            recv_sem=suf_sem.at[1, c],
            device_id=(group, partner),
            device_id_type=MESH,
        )

    def y_copy(c):
        return pltpu.make_async_remote_copy(
            src_ref=y_s.at[:, rows_of(c)],
            dst_ref=y_r.at[:, rows_of(c)],
            send_sem=y_sem.at[0, c],
            recv_sem=y_sem.at[1, c],
            device_id=device(across),
            device_id_type=MESH,
        )

    def ystat_copy(c):
        return pltpu.make_async_remote_copy(
            src_ref=ystat_s.at[c],
            dst_ref=ystat_r.at[c],
            send_sem=y_sem.at[2, c],
            recv_sem=y_sem.at[3, c],
            device_id=device(across),
            device_id_type=MESH,
        )

    def z_copy(c, step):
        dest = lax.rem(row + step, depth)
        return pltpu.make_async_remote_copy(
            src_ref=z_s.at[dest, rows_of(c)],
            dst_ref=z_r.at[row, rows_of(c)],
            send_sem=z_sem.at[0, step - 1, c],
            recv_sem=z_sem.at[1, step - 1, c],
            device_id=device(row_at(step)),
            device_id_type=MESH,
        )

    def zstat_copy(c, step):
        dest = lax.rem(row + step, depth)
        return pltpu.make_async_remote_copy(
            src_ref=zstat_s.at[dest, c],
            dst_ref=zstat_r.at[row, c],
            send_sem=z_sem.at[2, step - 1, c],
            recv_sem=z_sem.at[3, step - 1, c],
            device_id=device(row_at(step)),
            device_id_type=MESH,
        )

    def loop(count, body):
        def step(c, carry):
            body(c)
            return carry

        lax.fori_loop(0, count, step, 0)

    q_local().start()
    pool_local().start()
    loop(chunks, lambda c: suffix_local(c).start())
    pl.semaphore_wait(barrier, chips)

    def start_q(c):
        for step in range(1, depth):
            q_copy(c, step).start()
        q_copy(c, 0).start()
        suffix_remote(c).start()

    start_q(0)
    pool_remote().start()

    def start_later(c):
        start_q(c + 1)

    loop(chunks - 1, start_later)

    def forward(c):
        for step in range(1, depth):
            q_copy(c, step).wait_recv()
            q_forward(c, step).start()

    forward(0)
    q_local().wait()
    pool_local().wait()
    pool_remote().wait()

    lanes = lax.broadcasted_iota(jnp.int32, (heads, 128), 1)
    half_rows = depth * heads
    slot_ids = lax.broadcasted_iota(jnp.int32, (1, 2 * slots), 1) + me * (2 * slots)
    prefixes = order_ref.shape[1]
    per_prefix = blocks // prefixes

    def attend(q, request):
        chosen = prefix_ref[request]
        parts = []
        for side in range(2):
            for k in range(per_prefix):
                parts.append(pool_v[side, order_ref[side * per_prefix + k, chosen]])
        keys = jnp.concatenate(parts, axis=0)
        tails = jnp.concatenate([suffix_v[0, request], suffix_v[1, request]], axis=1)
        prefix_scores = lax.dot_general(
            q, keys, (((1,), (1,)), ((), ())), preferred_element_type=jnp.float32
        )
        suffix_scores = jnp.dot(q, tails, preferred_element_type=jnp.float32)
        live = slot_ids < length_ref[request]
        scores = jnp.concatenate(
            [
                prefix_scores * score_scale,
                jnp.where(live, suffix_scores * score_scale, -jnp.inf),
            ],
            axis=1,
        )
        highest = jnp.max(scores, axis=1, keepdims=True)
        weights = jnp.exp(scores - highest)
        total = jnp.sum(weights, axis=1, keepdims=True)
        rounded = weights.astype(jnp.bfloat16)
        split = keys.shape[0]
        mixed = jnp.dot(
            rounded[:, :split], keys[:, :LAT], preferred_element_type=jnp.float32
        ) + lax.dot_general(
            rounded[:, split:],
            tails[:LAT],
            (((1,), (1,)), ((), ())),
            preferred_element_type=jnp.float32,
        )
        return mixed / total, highest, total

    def do_chunk(c):
        @pl.when(c + 1 < chunks)
        def _():
            forward(c + 1)

        q_copy(c, 0).wait_recv()
        for step in range(1, depth):
            q_forward(c, step).wait_recv()
        suffix_local(c).wait()
        suffix_remote(c).wait()
        kept = jnp.zeros((heads, 128), jnp.float32)
        sent = jnp.zeros((heads, 128), jnp.float32)
        for half in range(chunk_pairs):
            pair = c * chunk_pairs + half
            q = q_v[:, :, pair].astype(jnp.float32).reshape(chips, 2, heads, q_v.shape[-1])
            outs = []
            for i in range(2):
                one = q[:, i].reshape(chips * heads, q_v.shape[-1]).astype(jnp.bfloat16)
                mixed, highest, total = attend(one, pair * 2 + i)
                for z in range(depth):
                    at = 2 * (z * REQ_CHUNK + half * 2 + i)
                    low = slice(z * heads, (z + 1) * heads)
                    high = slice(half_rows + z * heads, half_rows + (z + 1) * heads)
                    kept = jnp.where(lanes == at, highest[low], kept)
                    kept = jnp.where(lanes == at + 1, total[low], kept)
                    sent = jnp.where(lanes == at, highest[high], sent)
                    sent = jnp.where(lanes == at + 1, total[high], sent)
                outs.append(mixed.reshape(2, depth, heads, LAT))
            kept_v[:, pair] = jnp.concatenate([outs[0][0], outs[1][0]], axis=1)
            y_s[:, pair] = jnp.concatenate([outs[0][1], outs[1][1]], axis=1).astype(jnp.bfloat16)
        kept_stat[c] = kept
        ystat_s[c] = sent
        y_copy(c).start()
        ystat_copy(c).start()

    def merge_columns(c):
        y_copy(c).wait_recv()
        ystat_copy(c).wait_recv()
        ours = kept_stat[c]
        theirs = ystat_r[c]
        for z in range(depth):
            stats = jnp.zeros((heads, 128), jnp.float32)
            for half in range(chunk_pairs):
                pair = c * chunk_pairs + half
                mine = kept_v[z, pair]
                other = y_r[z, pair].astype(jnp.float32)
                outs = []
                for i in range(2):
                    at = 2 * (z * REQ_CHUNK + half * 2 + i)
                    top_a = ours[:, at : at + 1]
                    top_b = theirs[:, at : at + 1]
                    top = jnp.maximum(top_a, top_b)
                    part_a = jnp.exp(top_a - top) * ours[:, at + 1 : at + 2]
                    part_b = jnp.exp(top_b - top) * theirs[:, at + 1 : at + 2]
                    total = part_a + part_b
                    low = slice(i * heads, (i + 1) * heads)
                    outs.append(mine[low] * (part_a / total) + other[low] * (part_b / total))
                    to = 2 * (half * 2 + i)
                    stats = jnp.where(lanes == to, top, stats)
                    stats = jnp.where(lanes == to + 1, total, stats)
                both = jnp.concatenate(outs, axis=0)
                kept_v[z, pair] = both
                z_s[z, pair] = both.astype(jnp.bfloat16)
            zstat_s[z, c] = stats
        for step in range(1, depth):
            z_copy(c, step).start()
            zstat_copy(c, step).start()

    def stage(c):
        @pl.when(c < chunks)
        def _():
            do_chunk(c)

        @pl.when(c >= LAG)
        def _():
            merge_columns(c - LAG)

    loop(chunks + LAG, stage)

    def finish(c):
        stats = [zstat_s[row, c]]
        for step in range(1, depth):
            z_copy(c, step).wait_recv()
            zstat_copy(c, step).wait_recv()
            stats.append(zstat_r[lax.rem(row + depth - step, depth), c])
        for half in range(chunk_pairs):
            pair = c * chunk_pairs + half
            both = [kept_v[row, pair]]
            for step in range(1, depth):
                both.append(z_r[lax.rem(row + depth - step, depth), pair].astype(jnp.float32))
            outs = []
            for i in range(2):
                at = 2 * (half * 2 + i)
                tops = [s[:, at : at + 1] for s in stats]
                top = functools.reduce(jnp.maximum, tops)
                shares = [
                    jnp.exp(t - top) * s[:, at + 1 : at + 2] for t, s in zip(tops, stats)
                ]
                total = functools.reduce(jnp.add, shares)
                low = slice(i * heads, (i + 1) * heads)
                outs.append(
                    functools.reduce(
                        jnp.add, [b[low] * (s / total) for b, s in zip(both, shares)]
                    )
                )
            out_ref[pair] = jnp.concatenate(outs, axis=0).astype(jnp.bfloat16)

    loop(chunks, finish)

    def drain(c):
        for step in range(depth):
            q_copy(c, step).wait_send()
        for step in range(1, depth):
            q_forward(c, step).wait_send()
        y_copy(c).wait_send()
        ystat_copy(c).wait_send()
        for step in range(1, depth):
            z_copy(c, step).wait_send()
            zstat_copy(c, step).wait_send()

    loop(chunks, drain)


def fused_body(seq, queries, prefix_pool, block_table, prefix_of, suffix_cache, suffix_len):
    blocks_here, block_rows, channels = prefix_pool.shape
    prefix_total = block_table.shape[0]
    requests, heads, _ = queries.shape
    slots = suffix_cache.shape[1]
    per_prefix = blocks_here // prefix_total
    chips = seq // 2
    depth = chips // 2
    chunks = requests // REQ_CHUNK
    pairs = requests // 2
    chip = lax.axis_index("seq") // 2

    sides = chip * 2 + lax.iota(jnp.int32, 2)
    here = (block_table // blocks_here)[None] == sides[:, None, None]
    before = jnp.tril(jnp.ones((block_table.shape[1],) * 2, jnp.int32), -1)
    rank = jnp.sum(here[:, :, None, :] * before, axis=3)
    pick = here[:, None] & (rank[:, None] == lax.iota(jnp.int32, per_prefix)[None, :, None, None])
    local = block_table - block_table // blocks_here * blocks_here
    order = jnp.sum(jnp.where(pick, local[None, None], 0), axis=3).reshape(2 * per_prefix, prefix_total)

    any_spec = pl.BlockSpec(memory_space=pltpu.HBM)
    smem = pl.BlockSpec(memory_space=pltpu.SMEM)
    dma = pltpu.SemaphoreType.DMA
    out = pl.pallas_call(
        functools.partial(kernel, chips),
        out_shape=jax.ShapeDtypeStruct((pairs, 2 * heads, LAT), jnp.bfloat16),
        in_specs=[smem, smem, smem, any_spec, any_spec, any_spec],
        out_specs=pl.BlockSpec(memory_space=pltpu.VMEM),
        scratch_shapes=[
            pltpu.VMEM((2, blocks_here, block_rows, channels), jnp.bfloat16),
            pltpu.VMEM((2, requests, channels, slots), jnp.bfloat16),
            pltpu.VMEM((2, depth, pairs, 2 * heads, channels), jnp.bfloat16),
            pltpu.VMEM((depth, pairs, 2 * heads, LAT), jnp.float32),
            pltpu.VMEM((chunks, heads, 128), jnp.float32),
            pltpu.VMEM((depth, pairs, 2 * heads, LAT), jnp.bfloat16),
            pltpu.VMEM((chunks, heads, 128), jnp.float32),
            pltpu.VMEM((depth, pairs, 2 * heads, LAT), jnp.bfloat16),
            pltpu.VMEM((chunks, heads, 128), jnp.float32),
            pltpu.VMEM((depth, pairs, 2 * heads, LAT), jnp.bfloat16),
            pltpu.VMEM((depth, chunks, heads, 128), jnp.float32),
            pltpu.VMEM((depth, pairs, 2 * heads, LAT), jnp.bfloat16),
            pltpu.VMEM((depth, chunks, heads, 128), jnp.float32),
            dma((2 + chunks,)),
            dma((2,)),
            dma((2, chunks)),
            dma((chips, chunks)),
            dma((chips, chunks)),
            dma((4, chunks)),
            dma((4, depth - 1, chunks)),
        ],
        compiler_params=pltpu.CompilerParams(
            collective_id=0, has_side_effects=True, vmem_limit_bytes=63 * 1024 * 1024
        ),
    )(
        order,
        prefix_of,
        suffix_len,
        queries.reshape(pairs, 2 * heads, channels),
        prefix_pool,
        jnp.swapaxes(suffix_cache, 1, 2),
    )
    return out.reshape(requests, heads, LAT)


def solution(mesh):
    seq = mesh.shape["seq"]
    wide = seq == 16
    local = functools.partial(fused_body, seq) if wide else body
    return jax.shard_map(
        local,
        mesh=mesh,
        in_specs=(
            P("groups", "seq", None),
            P(("groups", "seq"), None, None),
            P("groups", None),
            P("groups"),
            P("groups", "seq", None),
            P("groups"),
        ),
        out_specs=P("groups", "seq", None),
        check_vma=False,
    )
```

```python
import functools

import jax
import jax.numpy as jnp
from jax import lax
from jax.experimental import pallas as pl
from jax.experimental.pallas import tpu as pltpu
from jax.sharding import PartitionSpec as P

LAT = 512


score_scale = 192.0 ** (-0.5)


def body(queries, prefix_pool, block_table, prefix_of, suffix_cache, suffix_len):
    blocks_here, block_rows, channels = prefix_pool.shape
    prefix_total = block_table.shape[0]
    slots_here = suffix_cache.shape[1]
    position = lax.axis_index("seq")
    block_ids = position * blocks_here + lax.iota(jnp.int32, blocks_here)
    owners = jnp.any(block_table[:, :, None] == block_ids[None, None, :], axis=1)
    prefix_ids = lax.iota(jnp.int32, prefix_total)
    labels = jnp.sum(owners.astype(jnp.int32) * prefix_ids[:, None], axis=0)
    order = jnp.argsort(labels, stable=True)
    segment_rows = blocks_here // prefix_total * block_rows
    segments = prefix_pool[order].reshape(prefix_total, segment_rows, channels)
    request_keys = jnp.concatenate([segments[prefix_of], suffix_cache], axis=1)
    slot_ids = position * slots_here + lax.iota(jnp.int32, slots_here)
    live_slots = slot_ids[None, :] < suffix_len[:, None]
    visible = jnp.concatenate(
        [jnp.ones((live_slots.shape[0], segment_rows), bool), live_slots], axis=1
    )
    scores = (
        jnp.einsum(
            "rhw,rkw->rhk",
            lax.all_gather(queries, "seq", axis=1, tiled=True),
            request_keys,
            preferred_element_type=jnp.float32,
        )
        * score_scale
    )
    scores = jnp.where(visible[:, None, :], scores, -jnp.inf)
    highest = lax.pmax(jnp.max(scores, axis=2), "seq")
    weights = jnp.exp(scores - highest[:, :, None])
    weight_sum = jnp.sum(weights, axis=2)
    rounded = weights.astype(jnp.bfloat16)
    weighted = jnp.einsum(
        "rhk,rkl->rhl", rounded, request_keys[:, :, :LAT], preferred_element_type=jnp.float32
    )
    weight_sum, weighted = (
        lax.psum_scatter(weight_sum, "seq", scatter_dimension=1, tiled=True),
        lax.psum_scatter(weighted, "seq", scatter_dimension=1, tiled=True),
    )
    return (weighted / weight_sum[:, :, None]).astype(jnp.bfloat16)


MESH = pl.DeviceIdType.MESH
REQ_CHUNK = 4
LAG = 2


def kernel(
    chips,
    order_ref,
    prefix_ref,
    length_ref,
    q_hbm,
    pool_hbm,
    suffix_hbm,
    out_ref,
    pool_v,
    suffix_v,
    q_v,
    kept_v,
    kept_stat,
    y_s,
    ystat_s,
    y_r,
    ystat_r,
    z_s,
    zstat_s,
    z_r,
    zstat_r,
    local_sem,
    pool_sem,
    suf_sem,
    q_send,
    q_recv,
    y_sem,
    z_sem,
):
    group = lax.axis_index("groups")
    position = lax.axis_index("seq")
    core = lax.rem(position, 2)
    me = lax.div(position, 2)
    column = lax.rem(me, 2)
    depth = chips // 2
    row = lax.div(me, 2)
    partner = position + 1 - 2 * core
    across = me + 1 - 2 * column
    twin = row + 1 - 2 * lax.rem(row, 2)

    def device(chip):
        return (group, chip * 2 + core)

    def chip_at(step):
        return lax.rem(me + step, chips)

    def row_at(step):
        return lax.rem(row + step, depth) * 2 + column

    blocks = pool_hbm.shape[0]
    requests = suffix_hbm.shape[0]
    slots = suffix_hbm.shape[2]
    pairs = q_hbm.shape[0]
    heads = q_hbm.shape[1] // 2
    chunks = requests // REQ_CHUNK
    chunk_pairs = REQ_CHUNK // 2

    barrier = pltpu.get_barrier_semaphore()
    pl.semaphore_signal(barrier, inc=1, device_id=(group, partner), device_id_type=MESH)
    for step in range(1, chips):
        pl.semaphore_signal(
            barrier, inc=1, device_id=device(chip_at(step)), device_id_type=MESH
        )

    def rows_of(c):
        return pl.ds(c * chunk_pairs, chunk_pairs)

    def reqs_of(c):
        return pl.ds(c * REQ_CHUNK, REQ_CHUNK)

    def q_local():
        return pltpu.make_async_copy(q_hbm, q_v.at[0, row], local_sem.at[0])

    def pool_local():
        return pltpu.make_async_copy(pool_hbm, pool_v.at[core], local_sem.at[1])

    def suffix_local(c):
        return pltpu.make_async_copy(
            suffix_hbm.at[reqs_of(c)], suffix_v.at[core, reqs_of(c)], local_sem.at[2 + c]
        )

    def q_move(c, side, source, kind, dest, to_side, fresh=False):
        held = q_hbm.at[rows_of(c)] if fresh else q_v.at[side, source, rows_of(c)]
        return pltpu.make_async_remote_copy(
            src_ref=held,
            dst_ref=q_v.at[to_side, source, rows_of(c)],
            send_sem=q_send.at[kind, c],
            recv_sem=q_recv.at[to_side * depth + source, c],
            device_id=device(dest),
            device_id_type=MESH,
        )

    def q_up(c, source, fresh=False):
        return q_move(c, 0, source, source, me + 2, 0, fresh)

    def q_down(c, source, fresh=False):
        return q_move(c, 0, source, depth + source, me - 2, 0, fresh)

    def q_across(c, source, fresh=False):
        return q_move(c, 0, source, 2 * depth + source, across, 1, fresh)

    def q_swap(c):
        return q_move(c, 1, row, 3 * depth, twin * 2 + column, 1)

    def q_arrival(c, side, source):
        return q_move(c, side, source, 0, across, side)

    def pool_remote():
        return pltpu.make_async_remote_copy(
            src_ref=pool_hbm,
            dst_ref=pool_v.at[core],
            send_sem=pool_sem.at[0],
            recv_sem=pool_sem.at[1],
            device_id=(group, partner),
            device_id_type=MESH,
        )

    def suffix_remote(c):
        return pltpu.make_async_remote_copy(
            src_ref=suffix_hbm.at[reqs_of(c)],
            dst_ref=suffix_v.at[core, reqs_of(c)],
            send_sem=suf_sem.at[0, c],
            recv_sem=suf_sem.at[1, c],
            device_id=(group, partner),
            device_id_type=MESH,
        )

    def y_copy(c):
        return pltpu.make_async_remote_copy(
            src_ref=y_s.at[:, rows_of(c)],
            dst_ref=y_r.at[:, rows_of(c)],
            send_sem=y_sem.at[0, c],
            recv_sem=y_sem.at[1, c],
            device_id=device(across),
            device_id_type=MESH,
        )

    def ystat_copy(c):
        return pltpu.make_async_remote_copy(
            src_ref=ystat_s.at[c],
            dst_ref=ystat_r.at[c],
            send_sem=y_sem.at[2, c],
            recv_sem=y_sem.at[3, c],
            device_id=device(across),
            device_id_type=MESH,
        )

    def z_copy(c, step):
        dest = lax.rem(row + step, depth)
        return pltpu.make_async_remote_copy(
            src_ref=z_s.at[dest, rows_of(c)],
            dst_ref=z_r.at[row, rows_of(c)],
            send_sem=z_sem.at[0, step - 1, c],
            recv_sem=z_sem.at[1, step - 1, c],
            device_id=device(row_at(step)),
            device_id_type=MESH,
        )

    def zstat_copy(c, step):
        dest = lax.rem(row + step, depth)
        return pltpu.make_async_remote_copy(
            src_ref=zstat_s.at[dest, c],
            dst_ref=zstat_r.at[row, c],
            send_sem=z_sem.at[2, step - 1, c],
            recv_sem=z_sem.at[3, step - 1, c],
            device_id=device(row_at(step)),
            device_id_type=MESH,
        )

    def loop(count, body):
        def step(c, carry):
            body(c)
            return carry

        lax.fori_loop(0, count, step, 0)

    q_local().start()
    pool_local().start()
    loop(chunks, lambda c: suffix_local(c).start())
    pl.semaphore_wait(barrier, chips)

    def start_q(c):
        q_across(c, row, True).start()

        @pl.when(row + 1 < depth)
        def _():
            q_up(c, row, True).start()

        @pl.when(row > 0)
        def _():
            q_down(c, row, True).start()

        suffix_remote(c).start()

    def relay(c, distance):
        below, above = row - distance, row + distance

        @pl.when(below >= 0)
        def _():
            q_arrival(c, 0, below).wait_recv()

            @pl.when(row + 1 < depth)
            def _():
                q_up(c, below).start()

            @pl.when(below != twin)
            def _():
                q_across(c, below).start()

        @pl.when(above < depth)
        def _():
            q_arrival(c, 0, above).wait_recv()

            @pl.when(row > 0)
            def _():
                q_down(c, above).start()

            @pl.when(above != twin)
            def _():
                q_across(c, above).start()

    def relay_all(c):
        for distance in range(1, depth):
            at = c + depth - distance

            @pl.when((at >= 0) & (at < chunks))
            def _():
                if distance == 1:
                    q_arrival(at, 1, row).wait_recv()
                    q_swap(at).start()
                relay(at, distance)

    start_q(0)
    pool_remote().start()

    def start_later(c):
        start_q(c + 1)

    loop(chunks - 1, start_later)

    loop(depth - 1, lambda c: relay_all(c + 1 - depth))
    q_local().wait()
    pool_local().wait()
    pool_remote().wait()

    lanes = lax.broadcasted_iota(jnp.int32, (heads, 128), 1)
    half_rows = depth * heads
    slot_ids = lax.broadcasted_iota(jnp.int32, (1, 2 * slots), 1) + me * (2 * slots)
    prefixes = order_ref.shape[1]
    per_prefix = blocks // prefixes

    def attend(q, request):
        chosen = prefix_ref[request]
        parts = []
        for side in range(2):
            for k in range(per_prefix):
                parts.append(pool_v[side, order_ref[side * per_prefix + k, chosen]])
        keys = jnp.concatenate(parts, axis=0)
        tails = jnp.concatenate([suffix_v[0, request], suffix_v[1, request]], axis=1)
        prefix_scores = lax.dot_general(
            q, keys, (((1,), (1,)), ((), ())), preferred_element_type=jnp.float32
        )
        suffix_scores = jnp.dot(q, tails, preferred_element_type=jnp.float32)
        live = slot_ids < length_ref[request]
        scores = jnp.concatenate(
            [
                prefix_scores * score_scale,
                jnp.where(live, suffix_scores * score_scale, -jnp.inf),
            ],
            axis=1,
        )
        highest = jnp.max(scores, axis=1, keepdims=True)
        weights = jnp.exp(scores - highest)
        total = jnp.sum(weights, axis=1, keepdims=True)
        rounded = weights.astype(jnp.bfloat16)
        split = keys.shape[0]
        mixed = jnp.dot(
            rounded[:, :split], keys[:, :LAT], preferred_element_type=jnp.float32
        ) + lax.dot_general(
            rounded[:, split:],
            tails[:LAT],
            (((1,), (1,)), ((), ())),
            preferred_element_type=jnp.float32,
        )
        return mixed / total, highest, total

    def do_chunk(c):
        for source in range(depth):

            @pl.when(row != source)
            def _():
                q_arrival(c, 1, source).wait_recv()

        suffix_local(c).wait()
        suffix_remote(c).wait()
        kept = jnp.zeros((heads, 128), jnp.float32)
        sent = jnp.zeros((heads, 128), jnp.float32)
        for half in range(chunk_pairs):
            pair = c * chunk_pairs + half
            q = q_v[:, :, pair].astype(jnp.float32).reshape(chips, 2, heads, q_v.shape[-1])
            outs = []
            for i in range(2):
                one = q[:, i].reshape(chips * heads, q_v.shape[-1]).astype(jnp.bfloat16)
                mixed, highest, total = attend(one, pair * 2 + i)
                for z in range(depth):
                    at = 2 * (z * REQ_CHUNK + half * 2 + i)
                    low = slice(z * heads, (z + 1) * heads)
                    high = slice(half_rows + z * heads, half_rows + (z + 1) * heads)
                    kept = jnp.where(lanes == at, highest[low], kept)
                    kept = jnp.where(lanes == at + 1, total[low], kept)
                    sent = jnp.where(lanes == at, highest[high], sent)
                    sent = jnp.where(lanes == at + 1, total[high], sent)
                outs.append(mixed.reshape(2, depth, heads, LAT))
            kept_v[:, pair] = jnp.concatenate([outs[0][0], outs[1][0]], axis=1)
            y_s[:, pair] = jnp.concatenate([outs[0][1], outs[1][1]], axis=1).astype(jnp.bfloat16)
        kept_stat[c] = kept
        ystat_s[c] = sent
        y_copy(c).start()
        ystat_copy(c).start()

    def merge_columns(c):
        y_copy(c).wait_recv()
        ystat_copy(c).wait_recv()
        ours = kept_stat[c]
        theirs = ystat_r[c]
        for z in range(depth):
            stats = jnp.zeros((heads, 128), jnp.float32)
            for half in range(chunk_pairs):
                pair = c * chunk_pairs + half
                mine = kept_v[z, pair]
                other = y_r[z, pair].astype(jnp.float32)
                outs = []
                for i in range(2):
                    at = 2 * (z * REQ_CHUNK + half * 2 + i)
                    top_a = ours[:, at : at + 1]
                    top_b = theirs[:, at : at + 1]
                    top = jnp.maximum(top_a, top_b)
                    part_a = jnp.exp(top_a - top) * ours[:, at + 1 : at + 2]
                    part_b = jnp.exp(top_b - top) * theirs[:, at + 1 : at + 2]
                    total = part_a + part_b
                    low = slice(i * heads, (i + 1) * heads)
                    outs.append(mine[low] * (part_a / total) + other[low] * (part_b / total))
                    to = 2 * (half * 2 + i)
                    stats = jnp.where(lanes == to, top, stats)
                    stats = jnp.where(lanes == to + 1, total, stats)
                both = jnp.concatenate(outs, axis=0)
                kept_v[z, pair] = both
                z_s[z, pair] = both.astype(jnp.bfloat16)
            zstat_s[z, c] = stats
        for step in range(1, depth):
            z_copy(c, step).start()
            zstat_copy(c, step).start()

    def stage(c):
        relay_all(c)

        @pl.when(c < chunks)
        def _():
            do_chunk(c)

        @pl.when(c >= LAG)
        def _():
            merge_columns(c - LAG)

    loop(chunks + LAG, stage)

    def finish(c):
        stats = [zstat_s[row, c]]
        for step in range(1, depth):
            z_copy(c, step).wait_recv()
            zstat_copy(c, step).wait_recv()
            stats.append(zstat_r[lax.rem(row + depth - step, depth), c])
        for half in range(chunk_pairs):
            pair = c * chunk_pairs + half
            both = [kept_v[row, pair]]
            for step in range(1, depth):
                both.append(z_r[lax.rem(row + depth - step, depth), pair].astype(jnp.float32))
            outs = []
            for i in range(2):
                at = 2 * (half * 2 + i)
                tops = [s[:, at : at + 1] for s in stats]
                top = functools.reduce(jnp.maximum, tops)
                shares = [
                    jnp.exp(t - top) * s[:, at + 1 : at + 2] for t, s in zip(tops, stats)
                ]
                total = functools.reduce(jnp.add, shares)
                low = slice(i * heads, (i + 1) * heads)
                outs.append(
                    functools.reduce(
                        jnp.add, [b[low] * (s / total) for b, s in zip(both, shares)]
                    )
                )
            out_ref[pair] = jnp.concatenate(outs, axis=0).astype(jnp.bfloat16)

    loop(chunks, finish)

    def drain(c):
        for source in range(depth):

            @pl.when((source <= row) & (row + 1 < depth))
            def _():
                q_up(c, source).wait_send()

            @pl.when((source >= row) & (row > 0))
            def _():
                q_down(c, source).wait_send()

            @pl.when(source != twin)
            def _():
                q_across(c, source).wait_send()

        q_swap(c).wait_send()
        y_copy(c).wait_send()
        ystat_copy(c).wait_send()
        for step in range(1, depth):
            z_copy(c, step).wait_send()
            zstat_copy(c, step).wait_send()

    loop(chunks, drain)


def fused_body(seq, queries, prefix_pool, block_table, prefix_of, suffix_cache, suffix_len):
    blocks_here, block_rows, channels = prefix_pool.shape
    prefix_total = block_table.shape[0]
    requests, heads, _ = queries.shape
    slots = suffix_cache.shape[1]
    per_prefix = blocks_here // prefix_total
    chips = seq // 2
    depth = chips // 2
    chunks = requests // REQ_CHUNK
    pairs = requests // 2
    chip = lax.axis_index("seq") // 2

    sides = chip * 2 + lax.iota(jnp.int32, 2)
    here = (block_table // blocks_here)[None] == sides[:, None, None]
    before = jnp.tril(jnp.ones((block_table.shape[1],) * 2, jnp.int32), -1)
    rank = jnp.sum(here[:, :, None, :] * before, axis=3)
    pick = here[:, None] & (rank[:, None] == lax.iota(jnp.int32, per_prefix)[None, :, None, None])
    local = block_table - block_table // blocks_here * blocks_here
    order = jnp.sum(jnp.where(pick, local[None, None], 0), axis=3).reshape(2 * per_prefix, prefix_total)

    any_spec = pl.BlockSpec(memory_space=pltpu.HBM)
    smem = pl.BlockSpec(memory_space=pltpu.SMEM)
    dma = pltpu.SemaphoreType.DMA
    out = pl.pallas_call(
        functools.partial(kernel, chips),
        out_shape=jax.ShapeDtypeStruct((pairs, 2 * heads, LAT), jnp.bfloat16),
        in_specs=[smem, smem, smem, any_spec, any_spec, any_spec],
        out_specs=pl.BlockSpec(memory_space=pltpu.VMEM),
        scratch_shapes=[
            pltpu.VMEM((2, blocks_here, block_rows, channels), jnp.bfloat16),
            pltpu.VMEM((2, requests, channels, slots), jnp.bfloat16),
            pltpu.VMEM((2, depth, pairs, 2 * heads, channels), jnp.bfloat16),
            pltpu.VMEM((depth, pairs, 2 * heads, LAT), jnp.float32),
            pltpu.VMEM((chunks, heads, 128), jnp.float32),
            pltpu.VMEM((depth, pairs, 2 * heads, LAT), jnp.bfloat16),
            pltpu.VMEM((chunks, heads, 128), jnp.float32),
            pltpu.VMEM((depth, pairs, 2 * heads, LAT), jnp.bfloat16),
            pltpu.VMEM((chunks, heads, 128), jnp.float32),
            pltpu.VMEM((depth, pairs, 2 * heads, LAT), jnp.bfloat16),
            pltpu.VMEM((depth, chunks, heads, 128), jnp.float32),
            pltpu.VMEM((depth, pairs, 2 * heads, LAT), jnp.bfloat16),
            pltpu.VMEM((depth, chunks, heads, 128), jnp.float32),
            dma((2 + chunks,)),
            dma((2,)),
            dma((2, chunks)),
            dma((3 * depth + 1, chunks)),
            dma((chips, chunks)),
            dma((4, chunks)),
            dma((4, depth - 1, chunks)),
        ],
        compiler_params=pltpu.CompilerParams(
            collective_id=0, has_side_effects=True, vmem_limit_bytes=63 * 1024 * 1024
        ),
    )(
        order,
        prefix_of,
        suffix_len,
        queries.reshape(pairs, 2 * heads, channels),
        prefix_pool,
        jnp.swapaxes(suffix_cache, 1, 2),
    )
    return out.reshape(requests, heads, LAT)


def solution(mesh):
    seq = mesh.shape["seq"]
    wide = seq == 16
    local = functools.partial(fused_body, seq) if wide else body
    return jax.shard_map(
        local,
        mesh=mesh,
        in_specs=(
            P("groups", "seq", None),
            P(("groups", "seq"), None, None),
            P("groups", None),
            P("groups"),
            P("groups", "seq", None),
            P("groups"),
        ),
        out_specs=P("groups", "seq", None),
        check_vma=False,
    )
```
